32 devices in a mesh: vocab: 32 (over z, y, x, core).
Axes of the slice: x: 2, y: 2, z: 4, core: 2. Of those that a mesh axis runs over, the one named last changes fastest.
Arguments:
- hidden: bfloat16 [2, 256, 3584], P(None, 'vocab'), may hold values from -256 to 256
- head_weight: bfloat16 [3584, 24576], P(None, 'vocab'), may hold values from -1 to 1
- teacher: bfloat16 [2, 256, 24576], P(None, None, 'vocab'), may hold values from 0 to 1
Outputs:
- token_loss: float32 [2, 256], P(None, 'vocab')
- hidden_grad: bfloat16 [2, 256, 3584], P(None, 'vocab')
- head_grad: bfloat16 [3584, 24576], P(None, 'vocab')
The draws below stay inside these ranges and needn't reach their ends.
All inputs are finite; a program needn't handle non-finite values.
Results may differ from the reference program's by a relative error of at most 0.012.
Values may be sent and summed in bfloat16 or wider, within the bound.
No kernel may reach another device: no remote copies, remote signals or barrier semaphores. Data moves between devices by JAX's collectives and lax.ppermute only.
A program may use at most 128 MiB of HBM per device.

```python
import math
import jax
import jax.numpy as jnp
from jax import lax

D = 3584
GROUP = 256
GROUPS = 2
VOCAB = 24576


def draw_head_weight(key, part):
    key_base, key_scale = jax.random.split(jax.random.fold_in(key, 11), 2)
    column_scale = jnp.exp(jax.random.uniform(key_scale, (1, VOCAB), minval=math.log(0.3), maxval=math.log(3.0)))
    base = jnp.clip(jax.random.normal(key_base, (D, VOCAB)), -6.0, 6.0)
    weight = base * column_scale / math.sqrt(D)
    return jnp.clip(weight, -1.0, 1.0).astype(jnp.bfloat16)


def draw_hidden(key, part):
    key_base, key_scale = jax.random.split(jax.random.fold_in(key, 13), 2)
    base = jnp.clip(jax.random.normal(key_base, (GROUPS, GROUP, D)), -6.0, 6.0)
    row_scale = jnp.exp(jax.random.uniform(key_scale, (GROUPS, GROUP, 1), minval=math.log(0.05), maxval=math.log(0.5)))
    states = (base * row_scale).reshape(GROUPS * GROUP, D)
    return states.reshape(GROUPS, GROUP, D).astype(jnp.bfloat16)


def draw_teacher(key, part):
    key_raw, key_weight = jax.random.split(jax.random.fold_in(key, 17), 2)
    position = jnp.arange(VOCAB, dtype=jnp.float32) / VOCAB
    raw = 2.0 * jnp.clip(jax.random.normal(key_raw, (GROUPS, GROUP, VOCAB)), -6.0, 6.0)
    log_mean = 2.0
    rising = math.log(3.0)
    shift_value = log_mean + math.log(VOCAB) + math.log((math.exp(rising) - 1.0) / rising)
    token_weight = jax.random.uniform(key_weight, (GROUPS, GROUP, 1), minval=0.5, maxval=1.5)
    probable = token_weight * jnp.exp(raw + rising * position - shift_value)
    return jnp.clip(probable, 0.0, 1.0).astype(jnp.bfloat16)


def setup_inputs(seed: int = 0) -> dict:
    splits = jax.random.split(jax.random.key(seed), 4)
    hidden = draw_hidden(jax.random.fold_in(splits[3], 71), 0)
    head_weight = draw_head_weight(jax.random.fold_in(splits[3], 71), 0)
    teacher = draw_teacher(jax.random.fold_in(splits[3], 71), 0)
    return {"hidden": hidden, "head_weight": head_weight, "teacher": teacher}


def reference(hidden, head_weight, teacher):
    loss_list = []
    hidden_list = []
    weight_grad = jnp.zeros(head_weight.shape, jnp.bfloat16)
    for group_index in range(GROUPS):
        logit_block = jnp.dot(hidden[group_index], head_weight, preferred_element_type=jnp.float32)
        target_wide = teacher[group_index].astype(jnp.float32)
        peak_logit = jnp.max(logit_block, axis=-1, keepdims=True)
        exp_total = jnp.sum(jnp.exp(logit_block - peak_logit), axis=-1, keepdims=True)
        log_norm = peak_logit + jnp.log(exp_total)
        teacher_mass = jnp.sum(target_wide, axis=-1, keepdims=True)
        cross_term = jnp.sum(target_wide * logit_block, axis=-1, keepdims=True)
        loss_list.append((teacher_mass * log_norm - cross_term)[:, 0])
        logit_grad = (teacher_mass * jnp.exp(logit_block - log_norm) - target_wide).astype(jnp.bfloat16)
        hidden_list.append(jnp.dot(logit_grad, head_weight.T, preferred_element_type=jnp.float32).astype(jnp.bfloat16))
        product_term = lax.dot_general(hidden[group_index], logit_grad, (((0,), (0,)), ((), ())), preferred_element_type=jnp.float32)
        weight_grad = (weight_grad.astype(jnp.float32) + product_term).astype(jnp.bfloat16)
    return (jnp.stack(loss_list), jnp.stack(hidden_list), weight_grad)
```

```python
import functools

import jax
import jax.numpy as jnp
from jax import lax
from jax.experimental import pallas as pl
from jax.experimental.pallas import tpu as pltpu
from jax.sharding import PartitionSpec as P

AXIS = "vocab"
ROW_TILE = 8


def stage_orders(size):
    bits = list(range(size.bit_length() - 2, 0, -1))
    low, high = [], []
    for start in range(0, len(bits), 2):
        pair = bits[start : start + 2]
        low += pair[::-1]
        high += pair
    return low, high


def masks_of(order):
    masks = [0]
    for bit in order:
        masks += [mask | (1 << bit) for mask in masks]
    return masks


def owner_of(me, masks, block):
    half = len(masks[0])
    core = lax.rem(me, 2)
    if block < half:
        return me ^ jnp.where(core == 0, masks[0][block], masks[1][block])
    block -= half
    return me ^ 1 ^ jnp.where(core == 0, masks[1][block], masks[0][block])


def swap(value, order_pair, stage, size):
    pairs = [(i, i ^ (1 << order_pair[i & 1][stage])) for i in range(size)]
    return lax.ppermute(value, AXIS, pairs)


def swap_core(value, size):
    return lax.ppermute(value, AXIS, [(i, i ^ 1) for i in range(size)])


def stats_kernel(masks, me_ref, own_ref, pair_ref, teacher_ref, out_ref):
    me = me_ref[0]
    groups = own_ref.shape[0]
    half = len(masks[0])
    size = 2 * half
    lane = lax.broadcasted_iota(jnp.int32, (ROW_TILE, groups * size), 1)
    norm_all = jnp.zeros((ROW_TILE, groups * size), jnp.float32)
    mass_all = norm_all
    cross_all = norm_all
    for block in range(size):
        owner = owner_of(me, masks, block)
        start = pl.multiple_of(owner * ROW_TILE, ROW_TILE)
        source = own_ref if block < half else pair_ref
        rows = pl.ds((block % half) * ROW_TILE, ROW_TILE)
        for group in range(groups):
            logits = source[group, rows, :]
            target = teacher_ref[group, pl.ds(start, ROW_TILE), :].astype(jnp.float32)
            peak = jnp.max(logits, axis=1, keepdims=True)
            total = jnp.sum(jnp.exp(logits - peak), axis=1, keepdims=True)
            mass = jnp.sum(target, axis=1, keepdims=True)
            cross = jnp.sum(target * logits, axis=1, keepdims=True)
            here = lane == group * size + owner
            norm_all = jnp.where(here, peak + jnp.log(total), norm_all)
            mass_all = jnp.where(here, mass, mass_all)
            cross_all = jnp.where(here, cross, cross_all)
    out_ref[0] = norm_all
    out_ref[1] = mass_all
    out_ref[2] = cross_all


def grad_kernel(masks, me_ref, stats_ref, own_ref, pair_ref, teacher_ref, loss_ref, own_grad_ref, pair_grad_ref):
    me = me_ref[0]
    groups = own_ref.shape[0]
    half = len(masks[0])
    size = 2 * half
    norms = stats_ref[:, 0]
    peak = jnp.max(norms, axis=0)
    log_norm = peak + jnp.log(jnp.sum(jnp.exp(norms - peak[None]), axis=0))
    mass = jnp.sum(stats_ref[:, 1], axis=0)
    cross = jnp.sum(stats_ref[:, 2], axis=0)
    loss_ref[...] = mass * log_norm - cross
    lane = lax.broadcasted_iota(jnp.int32, mass.shape, 1)
    for block in range(size):
        owner = owner_of(me, masks, block)
        start = pl.multiple_of(owner * ROW_TILE, ROW_TILE)
        source = own_ref if block < half else pair_ref
        result = own_grad_ref if block < half else pair_grad_ref
        rows = pl.ds((block % half) * ROW_TILE, ROW_TILE)
        for group in range(groups):
            here = lane == group * size + owner
            norm_rows = jnp.sum(jnp.where(here, log_norm, 0.0), axis=1, keepdims=True)
            mass_rows = jnp.sum(jnp.where(here, mass, 0.0), axis=1, keepdims=True)
            target = teacher_ref[group, pl.ds(start, ROW_TILE), :].astype(jnp.float32)
            grad = mass_rows * jnp.exp(source[group, rows, :] - norm_rows) - target
            result[group, rows, :] = grad.astype(jnp.bfloat16)


def vmem(count):
    return [pl.BlockSpec(memory_space=pltpu.VMEM)] * count


def call_stats(me, own, pair, teacher, masks):
    size = 2 * len(masks[0])
    return pl.pallas_call(
        functools.partial(stats_kernel, masks),
        out_shape=jax.ShapeDtypeStruct((3, ROW_TILE, own.shape[0] * size), jnp.float32),
        in_specs=[pl.BlockSpec(memory_space=pltpu.SMEM)] + vmem(3),
        out_specs=vmem(1)[0],
        cost_estimate=pl.CostEstimate(flops=2_000_000, bytes_accessed=2_400_000, transcendentals=400_000),
        name="stats",
    )(me, own, pair, teacher)


def call_grad(me, stats, own, pair, teacher, masks):
    grad = jax.ShapeDtypeStruct(own.shape, jnp.bfloat16)
    return pl.pallas_call(
        functools.partial(grad_kernel, masks),
        out_shape=(jax.ShapeDtypeStruct(stats.shape[2:], jnp.float32), grad, grad),
        in_specs=[pl.BlockSpec(memory_space=pltpu.SMEM)] + vmem(4),
        out_specs=tuple(vmem(3)),
        cost_estimate=pl.CostEstimate(flops=2_000_000, bytes_accessed=3_200_000, transcendentals=400_000),
        name="grad",
    )(me, stats, own, pair, teacher)


def plain_stats(owners, own, pair, teacher):
    groups, _, row_count, width = teacher.shape
    logits = jnp.concatenate([own, pair], axis=1).reshape(groups, -1, row_count, width)
    target = jnp.take(teacher, owners, axis=1).astype(jnp.float32)
    peak = jnp.max(logits, axis=-1)
    norm = peak + jnp.log(jnp.sum(jnp.exp(logits - peak[..., None]), axis=-1))
    stats = jnp.stack([norm, jnp.sum(target, axis=-1), jnp.sum(target * logits, axis=-1)])
    return jnp.zeros_like(stats).at[:, :, owners].set(stats)


def plain_grad(owners, stats, own, pair, teacher):
    groups, size, row_count, width = teacher.shape
    logits = jnp.concatenate([own, pair], axis=1).reshape(groups, size, row_count, width)
    norms = stats[:, 0]
    log_norm = jax.nn.logsumexp(norms, axis=0)
    mass = jnp.sum(stats[:, 1], axis=0)
    loss = mass * log_norm - jnp.sum(stats[:, 2], axis=0)
    target = jnp.take(teacher, owners, axis=1).astype(jnp.float32)
    scale = jnp.take(mass, owners, axis=1)[..., None]
    grad = scale * jnp.exp(logits - jnp.take(log_norm, owners, axis=1)[..., None]) - target
    grad = grad.astype(jnp.bfloat16).reshape(groups, size * row_count, width)
    return loss, grad[:, : size * row_count // 2], grad[:, size * row_count // 2 :]


def exchange_stats(stats, size):
    spread = jnp.broadcast_to(stats[None], (size, *stats.shape))
    return lax.all_to_all(spread, AXIS, 0, 0, tiled=True)


def matmul(left, right, contract):
    return lax.dot_general(left, right, (contract, ((), ())), preferred_element_type=jnp.float32)


def shards(hidden, head_weight, teacher):
    groups, row_count, model_width = hidden.shape
    size = lax.axis_size(AXIS)
    me = lax.axis_index(AXIS)
    orders = stage_orders(size)
    masks = tuple(masks_of(order) for order in orders)
    tiled = row_count == ROW_TILE
    stages = len(orders[0])

    held = hidden
    for stage in range(stages):
        held = jnp.concatenate([held, swap(held, orders, stage, size)], axis=1)
    other = swap_core(held, size)

    half_rows = held.shape[1]
    width = head_weight.shape[1]

    def project(rows):
        flat = matmul(rows.reshape(-1, model_width), head_weight, ((1,), (0,)))
        return flat.reshape(groups, half_rows, width)

    own_logits = project(held)
    pair_logits = project(other)
    if tiled:
        me_ref = me.reshape(1)
        stats = exchange_stats(call_stats(me_ref, own_logits, pair_logits, teacher, masks), size)
        loss, own_grad, pair_grad = call_grad(me_ref, stats, own_logits, pair_logits, teacher, masks)
        own_loss = lax.dynamic_index_in_dim(
            loss.reshape(row_count, groups, size), me, axis=2, keepdims=False
        ).T
    else:
        owners = jnp.stack([owner_of(me, masks, block) for block in range(size)])
        blocks = teacher.reshape(groups, size, row_count, width)
        stats = exchange_stats(plain_stats(owners, own_logits, pair_logits, blocks), size)
        loss, own_grad, pair_grad = plain_grad(owners, stats, own_logits, pair_logits, blocks)
        own_loss = lax.dynamic_index_in_dim(loss, me, axis=1, keepdims=False)

    def pull_back(grad):
        flat = matmul(grad.reshape(-1, width), head_weight, ((1,), (1,)))
        return flat.reshape(groups, half_rows, model_width)

    sent = swap_core(pull_back(pair_grad).astype(jnp.bfloat16), size)
    total = (pull_back(own_grad) + sent.astype(jnp.float32)).astype(jnp.bfloat16)
    for stage in reversed(range(stages)):
        rows = total.shape[1] // 2
        got = swap(total[:, rows:], orders, stage, size)
        total = (total[:, :rows].astype(jnp.float32) + got.astype(jnp.float32)).astype(jnp.bfloat16)

    flat = lambda value: value.reshape(-1, value.shape[-1])
    weight_grad = matmul(flat(held), flat(own_grad), ((0,), (0,)))
    weight_grad = weight_grad + matmul(flat(other), flat(pair_grad), ((0,), (0,)))
    return (own_loss, total, weight_grad.astype(jnp.bfloat16))


def solution(mesh):
    in_specs = (P(None, AXIS, None), P(None, AXIS), P(None, None, AXIS))
    out_specs = (P(None, AXIS), P(None, AXIS, None), P(None, AXIS))
    return jax.shard_map(shards, mesh=mesh, in_specs=in_specs, out_specs=out_specs, check_vma=False)
```

```python
import functools

import jax
import jax.numpy as jnp
from jax import lax
from jax.experimental import pallas as pl
from jax.experimental.pallas import tpu as pltpu
from jax.sharding import PartitionSpec as P

AXIS = "vocab"
ROW_TILE = 8
VMEM_BYTES = 12 << 20


def stage_orders(size):
    bits = list(range(size.bit_length() - 2, 0, -1))
    low, high = [], []
    for start in range(0, len(bits), 2):
        pair = bits[start : start + 2]
        low += pair[::-1]
        high += pair
    return low, high


def masks_of(order):
    masks = [0]
    for bit in order:
        masks += [mask | (1 << bit) for mask in masks]
    return masks


def owner_of(me, masks, block):
    half = len(masks[0])
    core = lax.rem(me, 2)
    if block < half:
        return me ^ jnp.where(core == 0, masks[0][block], masks[1][block])
    block -= half
    return me ^ 1 ^ jnp.where(core == 0, masks[1][block], masks[0][block])


def swap(value, order_pair, stage, size):
    pairs = [(i, i ^ (1 << order_pair[i & 1][stage])) for i in range(size)]
    return lax.ppermute(value, AXIS, pairs)


def swap_core(value, size):
    return lax.ppermute(value, AXIS, [(i, i ^ 1) for i in range(size)])


def stats_kernel(masks, groups, me_ref, *refs):
    own_refs, pair_refs, (teacher_ref, out_ref) = refs[:groups], refs[groups : 2 * groups], refs[2 * groups :]
    me = me_ref[0]
    half = len(masks[0])
    size = 2 * half
    lane = lax.broadcasted_iota(jnp.int32, (ROW_TILE, groups * size), 1)
    norm_all = jnp.zeros((ROW_TILE, groups * size), jnp.float32)
    mass_all = norm_all
    cross_all = norm_all
    for block in range(size):
        owner = owner_of(me, masks, block)
        start = pl.multiple_of(owner * ROW_TILE, ROW_TILE)
        source = own_refs if block < half else pair_refs
        rows = pl.ds((block % half) * ROW_TILE, ROW_TILE)
        for group in range(groups):
            logits = source[group][rows, :]
            target = teacher_ref[group, pl.ds(start, ROW_TILE), :].astype(jnp.float32)
            peak = jnp.max(logits, axis=1, keepdims=True)
            total = jnp.sum(jnp.exp(logits - peak), axis=1, keepdims=True)
            mass = jnp.sum(target, axis=1, keepdims=True)
            cross = jnp.sum(target * logits, axis=1, keepdims=True)
            here = lane == group * size + owner
            norm_all = jnp.where(here, peak + jnp.log(total), norm_all)
            mass_all = jnp.where(here, mass, mass_all)
            cross_all = jnp.where(here, cross, cross_all)
    out_ref[0] = norm_all
    out_ref[1] = mass_all
    out_ref[2] = cross_all


def grad_kernel(masks, groups, me_ref, stats_ref, *refs):
    own_refs, pair_refs, refs = refs[:groups], refs[groups : 2 * groups], refs[2 * groups :]
    teacher_ref, loss_ref, refs = refs[0], refs[1], refs[2:]
    own_grad_refs, pair_grad_refs = refs[:groups], refs[groups:]
    me = me_ref[0]
    half = len(masks[0])
    size = 2 * half
    log_norm, mass, cross = stats_ref[0], stats_ref[1], stats_ref[2]
    loss_ref[...] = mass * log_norm - cross
    lane = lax.broadcasted_iota(jnp.int32, mass.shape, 1)
    for block in range(size):
        owner = owner_of(me, masks, block)
        start = pl.multiple_of(owner * ROW_TILE, ROW_TILE)
        source = own_refs if block < half else pair_refs
        result = own_grad_refs if block < half else pair_grad_refs
        rows = pl.ds((block % half) * ROW_TILE, ROW_TILE)
        for group in range(groups):
            here = lane == group * size + owner
            norm_rows = jnp.sum(jnp.where(here, log_norm, 0.0), axis=1, keepdims=True)
            mass_rows = jnp.sum(jnp.where(here, mass, 0.0), axis=1, keepdims=True)
            target = teacher_ref[group, pl.ds(start, ROW_TILE), :].astype(jnp.float32)
            grad = mass_rows * jnp.exp(source[group][rows, :] - norm_rows) - target
            result[group][rows, :] = grad.astype(jnp.bfloat16)


def vmem(count):
    return [pl.BlockSpec(memory_space=pltpu.VMEM)] * count


def call_stats(me, own, pair, teacher, masks):
    groups, size = len(own), 2 * len(masks[0])
    return pl.pallas_call(
        functools.partial(stats_kernel, masks, groups),
        out_shape=jax.ShapeDtypeStruct((3, ROW_TILE, groups * size), jnp.float32),
        in_specs=[pl.BlockSpec(memory_space=pltpu.SMEM)] + vmem(2 * groups + 1),
        out_specs=vmem(1)[0],
        cost_estimate=pl.CostEstimate(flops=2_000_000, bytes_accessed=2_400_000, transcendentals=400_000),
        compiler_params=pltpu.CompilerParams(vmem_limit_bytes=VMEM_BYTES),
        name="stats",
    )(me, *own, *pair, teacher)


def call_grad(me, stats, own, pair, teacher, masks):
    groups = len(own)
    grad = jax.ShapeDtypeStruct(own[0].shape, jnp.bfloat16)
    loss, *grads = pl.pallas_call(
        functools.partial(grad_kernel, masks, groups),
        out_shape=[jax.ShapeDtypeStruct(stats.shape[1:], jnp.float32)] + [grad] * (2 * groups),
        in_specs=[pl.BlockSpec(memory_space=pltpu.SMEM)] + vmem(2 * groups + 2),
        out_specs=vmem(2 * groups + 1),
        cost_estimate=pl.CostEstimate(flops=2_000_000, bytes_accessed=3_200_000, transcendentals=400_000),
        compiler_params=pltpu.CompilerParams(vmem_limit_bytes=VMEM_BYTES),
        name="grad",
    )(me, stats, *own, *pair, teacher)
    return loss, grads[:groups], grads[groups:]


def plain_stats(owners, own, pair, teacher):
    groups, _, row_count, width = teacher.shape
    logits = jnp.concatenate([own, pair], axis=1).reshape(groups, -1, row_count, width)
    target = jnp.take(teacher, owners, axis=1).astype(jnp.float32)
    peak = jnp.max(logits, axis=-1)
    norm = peak + jnp.log(jnp.sum(jnp.exp(logits - peak[..., None]), axis=-1))
    stats = jnp.stack([norm, jnp.sum(target, axis=-1), jnp.sum(target * logits, axis=-1)])
    return jnp.zeros_like(stats).at[:, :, owners].set(stats)


def plain_grad(owners, stats, own, pair, teacher):
    groups, size, row_count, width = teacher.shape
    logits = jnp.concatenate([own, pair], axis=1).reshape(groups, size, row_count, width)
    log_norm, mass, cross = stats
    loss = mass * log_norm - cross
    target = jnp.take(teacher, owners, axis=1).astype(jnp.float32)
    scale = jnp.take(mass, owners, axis=1)[..., None]
    grad = scale * jnp.exp(logits - jnp.take(log_norm, owners, axis=1)[..., None]) - target
    grad = grad.astype(jnp.bfloat16).reshape(groups, size * row_count, width)
    return loss, grad[:, : size * row_count // 2], grad[:, size * row_count // 2 :]


def merge_stats(left, right):
    plane = lax.broadcasted_iota(jnp.int32, left.shape, 0)
    high, low = jnp.maximum(left, right), jnp.minimum(left, right)
    return jnp.where(plane == 0, high + jnp.log1p(jnp.exp(low - high)), left + right)


def exchange_stats(stats, orders, size):
    stats = merge_stats(stats, swap_core(stats, size))
    for stage in range(len(orders[0])):
        stats = merge_stats(stats, swap(stats, orders, stage, size))
    return stats


def matmul(left, right, contract):
    return lax.dot_general(left, right, (contract, ((), ())), preferred_element_type=jnp.float32)


def shards(hidden, head_weight, teacher):
    groups, row_count, model_width = hidden.shape
    size = lax.axis_size(AXIS)
    me = lax.axis_index(AXIS)
    orders = stage_orders(size)
    masks = tuple(masks_of(order) for order in orders)
    tiled = row_count == ROW_TILE
    stages = len(orders[0])
    width = head_weight.shape[1]

    held = [lax.optimization_barrier(hidden[group]) for group in range(groups)]
    for stage in range(stages):
        got = [swap(rows, orders, stage, size) for rows in held]
        held = [lax.optimization_barrier(jnp.concatenate(pair, axis=0)) for pair in zip(held, got)]
    other = [swap_core(rows, size) for rows in held]

    own_logits = [matmul(rows, head_weight, ((1,), (0,))) for rows in held]
    pair_logits = [matmul(rows, head_weight, ((1,), (0,))) for rows in other]
    if tiled:
        me_ref = me.reshape(1)
        stats = exchange_stats(call_stats(me_ref, own_logits, pair_logits, teacher, masks), orders, size)
        loss, own_grad, pair_grad = call_grad(me_ref, stats, own_logits, pair_logits, teacher, masks)
        own_loss = lax.dynamic_index_in_dim(
            loss.reshape(row_count, groups, size), me, axis=2, keepdims=False
        ).T
    else:
        owners = jnp.stack([owner_of(me, masks, block) for block in range(size)])
        blocks = teacher.reshape(groups, size, row_count, width)
        own_all, pair_all = jnp.stack(own_logits), jnp.stack(pair_logits)
        stats = exchange_stats(plain_stats(owners, own_all, pair_all, blocks), orders, size)
        loss, own_grad, pair_grad = plain_grad(owners, stats, own_all, pair_all, blocks)
        own_loss = lax.dynamic_index_in_dim(loss, me, axis=1, keepdims=False)

    total = []
    for group in range(groups):
        sent = matmul(pair_grad[group], head_weight, ((1,), (1,))).astype(jnp.bfloat16)
        got = swap_core(sent, size)
        kept = matmul(own_grad[group], head_weight, ((1,), (1,)))
        total.append((kept + got.astype(jnp.float32)).astype(jnp.bfloat16))
    row_blocks = [block for pair in zip(held, other) for block in pair]
    grad_blocks = [block for pair in zip(own_grad, pair_grad) for block in pair]
    total, row_blocks, grad_blocks = lax.optimization_barrier((total, row_blocks, grad_blocks))
    weight_grad = matmul(jnp.concatenate(row_blocks), jnp.concatenate(grad_blocks), ((0,), (0,)))
    for stage in reversed(range(stages)):
        rows = total[0].shape[0] // 2
        got = [swap(part[rows:], orders, stage, size) for part in total]
        total = [
            (part[:rows].astype(jnp.float32) + add.astype(jnp.float32)).astype(jnp.bfloat16)
            for part, add in zip(total, got)
        ]

    return (own_loss, jnp.stack(total), weight_grad.astype(jnp.bfloat16))


def solution(mesh):
    in_specs = (P(None, AXIS, None), P(None, AXIS), P(None, None, AXIS))
    out_specs = (P(None, AXIS), P(None, AXIS, None), P(None, AXIS))
    return jax.shard_map(shards, mesh=mesh, in_specs=in_specs, out_specs=out_specs, check_vma=False)
```

```python
import functools

import jax
import jax.numpy as jnp
from jax import lax
from jax.experimental import pallas as pl
from jax.experimental.pallas import tpu as pltpu
from jax.sharding import PartitionSpec as P

AXIS = "vocab"
ROW_TILE = 8
STATS_RADIX_BITS = 2
VMEM_BYTES = 12 << 20


def stage_orders(size, groups):
    bits = list(range(size.bit_length() - 2, 0, -1))
    low, high = [], []
    for start in range(0, len(bits), 2):
        pair = bits[start : start + 2]
        low += pair if start == 0 else pair[::-1]
        high += pair[::-1] if start == 0 else pair
    return [[low, high] for _ in range(groups)]


def masks_of(order):
    masks = [0]
    for bit in order:
        masks += [mask | (1 << bit) for mask in masks]
    return tuple(masks)


def owner_of(me, masks, block):
    half = len(masks[0])
    core = lax.rem(me, 2)
    if block < half:
        return me ^ jnp.where(core == 0, masks[0][block], masks[1][block])
    block -= half
    return me ^ 1 ^ jnp.where(core == 0, masks[1][block], masks[0][block])


def swap(value, order_pair, stage, size):
    pairs = [(i, i ^ (1 << order_pair[i & 1][stage])) for i in range(size)]
    return lax.ppermute(value, AXIS, pairs)


def swap_core(value, size):
    return lax.ppermute(value, AXIS, [(i, i ^ 1) for i in range(size)])


def stats_kernel(masks, me_ref, teacher_ref, *refs):
    me = me_ref[0]
    groups = teacher_ref.shape[0]
    own_refs, pair_refs, out_ref = refs[:groups], refs[groups : 2 * groups], refs[2 * groups]
    half = len(masks[0][0])
    size = 2 * half
    lane = lax.broadcasted_iota(jnp.int32, (ROW_TILE, groups * size), 1)
    norm_all = jnp.zeros((ROW_TILE, groups * size), jnp.float32)
    mass_all = norm_all
    cross_all = norm_all
    for block in range(size):
        source = own_refs if block < half else pair_refs
        for group in range(groups):
            owner = owner_of(me, masks[group], block)
            start = pl.multiple_of(owner * ROW_TILE, ROW_TILE)
            logits = source[group][pl.ds((block % half) * ROW_TILE, ROW_TILE), :]
            target = teacher_ref[group, pl.ds(start, ROW_TILE), :].astype(jnp.float32)
            peak = jnp.max(logits, axis=1, keepdims=True)
            total = jnp.sum(jnp.exp(logits - peak), axis=1, keepdims=True)
            mass = jnp.sum(target, axis=1, keepdims=True)
            cross = jnp.sum(target * logits, axis=1, keepdims=True)
            here = lane == group * size + owner
            norm_all = jnp.where(here, peak + jnp.log(total), norm_all)
            mass_all = jnp.where(here, mass, mass_all)
            cross_all = jnp.where(here, cross, cross_all)
    out_ref[0] = norm_all
    out_ref[1] = mass_all
    out_ref[2] = cross_all


def grad_kernel(masks, me_ref, stats_ref, teacher_ref, *refs):
    me = me_ref[0]
    groups = teacher_ref.shape[0]
    own_refs, pair_refs = refs[:groups], refs[groups : 2 * groups]
    loss_ref, own_grad_ref, pair_grad_ref = refs[2 * groups :]
    half = len(masks[0][0])
    size = 2 * half
    log_norm, mass, cross = stats_ref[0], stats_ref[1], stats_ref[2]
    loss = mass * log_norm - cross
    lane = lax.broadcasted_iota(jnp.int32, mass.shape, 1)
    square = (ROW_TILE, ROW_TILE)
    diagonal = lax.broadcasted_iota(jnp.int32, square, 0) == lax.broadcasted_iota(jnp.int32, square, 1)
    for group in range(groups):
        column = jnp.sum(jnp.where(lane == group * size + me, loss, 0.0), axis=1, keepdims=True)
        loss_ref[pl.ds(group, 1), :] = jnp.sum(jnp.where(diagonal, column, 0.0), axis=0, keepdims=True)
    for block in range(size):
        source = own_refs if block < half else pair_refs
        result = own_grad_ref if block < half else pair_grad_ref
        for group in range(groups):
            owner = owner_of(me, masks[group], block)
            start = pl.multiple_of(owner * ROW_TILE, ROW_TILE)
            logits = source[group][pl.ds((block % half) * ROW_TILE, ROW_TILE), :]
            here = lane == group * size + owner
            norm_rows = jnp.sum(jnp.where(here, log_norm, 0.0), axis=1, keepdims=True)
            mass_rows = jnp.sum(jnp.where(here, mass, 0.0), axis=1, keepdims=True)
            target = teacher_ref[group, pl.ds(start, ROW_TILE), :].astype(jnp.float32)
            grad = mass_rows * jnp.exp(logits - norm_rows) - target
            result[pl.ds((group * half + block % half) * ROW_TILE, ROW_TILE), :] = grad.astype(jnp.bfloat16)


def vmem(count):
    return [pl.BlockSpec(memory_space=pltpu.VMEM)] * count


def call_stats(me, own, pair, teacher, masks):
    groups, size = teacher.shape[0], 2 * len(masks[0][0])
    return pl.pallas_call(
        functools.partial(stats_kernel, masks),
        out_shape=jax.ShapeDtypeStruct((3, ROW_TILE, groups * size), jnp.float32),
        in_specs=[pl.BlockSpec(memory_space=pltpu.SMEM)] + vmem(2 * groups + 1),
        out_specs=vmem(1)[0],
        cost_estimate=pl.CostEstimate(flops=2_000_000, bytes_accessed=2_400_000, transcendentals=400_000),
        compiler_params=pltpu.CompilerParams(vmem_limit_bytes=VMEM_BYTES),
        name="stats",
    )(me, teacher, *own, *pair)


def call_grad(me, stats, own, pair, teacher, masks):
    groups = len(own)
    grad = jax.ShapeDtypeStruct((groups * own[0].shape[0], own[0].shape[1]), jnp.bfloat16)
    return pl.pallas_call(
        functools.partial(grad_kernel, masks),
        out_shape=[jax.ShapeDtypeStruct((groups, ROW_TILE), jnp.float32), grad, grad],
        in_specs=[pl.BlockSpec(memory_space=pltpu.SMEM)] + vmem(2 * groups + 2),
        out_specs=vmem(3),
        cost_estimate=pl.CostEstimate(flops=2_000_000, bytes_accessed=3_200_000, transcendentals=400_000),
        compiler_params=pltpu.CompilerParams(vmem_limit_bytes=VMEM_BYTES),
        name="grad",
    )(me, stats, teacher, *own, *pair)


def joined(own, pair, size):
    parts = [jnp.stack(part).reshape(len(part), size // 2, -1, part[0].shape[-1]) for part in (own, pair)]
    return jnp.concatenate(parts, axis=1)


def taken(values, owners):
    return jnp.stack([jnp.take(value, owner, axis=0) for value, owner in zip(values, owners)])


def plain_stats(owners, own, pair, teacher):
    logits = joined(own, pair, teacher.shape[1])
    target = taken(teacher, owners).astype(jnp.float32)
    peak = jnp.max(logits, axis=-1)
    norm = peak + jnp.log(jnp.sum(jnp.exp(logits - peak[..., None]), axis=-1))
    stats = jnp.stack([norm, jnp.sum(target, axis=-1), jnp.sum(target * logits, axis=-1)])
    back = [jnp.zeros_like(stats[:, 0]).at[:, owner].set(stats[:, group]) for group, owner in enumerate(owners)]
    return jnp.stack(back, axis=1)


def plain_grad(me, owners, stats, own, pair, teacher):
    size, _, width = teacher.shape[1:]
    log_norm, mass, cross = stats
    loss = lax.dynamic_index_in_dim(mass * log_norm - cross, me, axis=1, keepdims=False)
    shifted = joined(own, pair, size) - taken(log_norm, owners)[..., None]
    grad = taken(mass, owners)[..., None] * jnp.exp(shifted) - taken(teacher, owners).astype(jnp.float32)
    grad = grad.astype(jnp.bfloat16)
    own_grad, pair_grad = grad[:, : size // 2], grad[:, size // 2 :]
    return loss, own_grad.reshape(-1, width), pair_grad.reshape(-1, width)


def merge_stats(left, right):
    plane = lax.broadcasted_iota(jnp.int32, left.shape, 0)
    high, low = jnp.maximum(left, right), jnp.minimum(left, right)
    return jnp.where(plane == 0, high + jnp.log1p(jnp.exp(low - high)), left + right)


def exchange_stats(stats, size):
    stats = merge_stats(stats, swap_core(stats, size))
    bits = list(range(1, size.bit_length() - 1))
    while bits:
        step, bits = bits[:STATS_RADIX_BITS], bits[STATS_RADIX_BITS:]
        got = [lax.ppermute(stats, AXIS, [(i, i ^ mask) for i in range(size)]) for mask in masks_of(step)[1:]]
        for value in got:
            stats = merge_stats(stats, value)
    return stats


def matmul(left, right, contract):
    return lax.dot_general(left, right, (contract, ((), ())), preferred_element_type=jnp.float32)


def add_round(left, right):
    return (left.astype(jnp.float32) + right.astype(jnp.float32)).astype(jnp.bfloat16)


def shards(hidden, head_weight, teacher):
    groups, row_count, _ = hidden.shape
    size = lax.axis_size(AXIS)
    me = lax.axis_index(AXIS)
    walks = stage_orders(size, groups)
    masks = [[masks_of(order) for order in walk] for walk in walks]
    stages = len(walks[0][0])
    width = head_weight.shape[1]

    held = [hidden[group] for group in range(groups)]
    for stage in range(stages):
        for group in range(groups):
            rows = lax.optimization_barrier(held[group])
            got = swap(rows, walks[group], stage, size)
            held[group] = jnp.concatenate([rows, got])
    held = [lax.optimization_barrier(rows) for rows in held]
    other, own, pair = [], [], []
    for group in range(groups):
        other.append(swap_core(held[group], size))
        own.append(matmul(held[group], head_weight, ((1,), (0,))))
        pair.append(matmul(other[group], head_weight, ((1,), (0,))))

    if row_count == ROW_TILE:
        stats = exchange_stats(call_stats(me.reshape(1), own, pair, teacher, masks), size)
        loss, own_grad, pair_grad = call_grad(me.reshape(1), stats, own, pair, teacher, masks)
    else:
        owners = [jnp.stack([owner_of(me, masks[group], block) for block in range(size)]) for group in range(groups)]
        blocks = teacher.reshape(groups, size, row_count, width)
        stats = exchange_stats(plain_stats(owners, own, pair, blocks), size)
        loss, own_grad, pair_grad = plain_grad(me, owners, stats, own, pair, blocks)

    sent = matmul(pair_grad, head_weight, ((1,), (1,))).astype(jnp.bfloat16)
    sent, mine = lax.optimization_barrier((sent, own_grad))
    kept = matmul(mine, head_weight, ((1,), (1,)))
    half = kept.shape[0] // groups
    kept = lax.optimization_barrier([kept[group * half : (group + 1) * half] for group in range(groups)])
    totals = []
    for group in range(groups):
        rows = slice(group * half, (group + 1) * half)
        got = swap_core(sent[rows], size)
        totals.append(add_round(kept[group], got))

    row_blocks = jnp.concatenate([*held, *other])
    grad_blocks = jnp.concatenate([own_grad, pair_grad])
    weight_grad = matmul(row_blocks, grad_blocks, ((0,), (0,)))

    for stage in reversed(range(stages)):
        rows = totals[0].shape[0] // 2
        for group in range(groups):
            got = swap(totals[group][rows:], walks[group], stage, size)
            totals[group] = add_round(totals[group][:rows], got)
    return (loss, jnp.stack(totals), weight_grad.astype(jnp.bfloat16))


def solution(mesh):
    in_specs = (P(None, AXIS, None), P(None, AXIS), P(None, None, AXIS))
    out_specs = (P(None, AXIS), P(None, AXIS, None), P(None, AXIS))

    return jax.shard_map(shards, mesh=mesh, in_specs=in_specs, out_specs=out_specs, check_vma=False)
```

```python
import functools

import jax
import jax.numpy as jnp
from jax import lax
from jax.experimental import pallas as pl
from jax.experimental.pallas import tpu as pltpu
from jax.sharding import PartitionSpec as P

AXIS = "vocab"
ROW_TILE = 8
STATS_RADIX_BITS = 2
VMEM_BYTES = 12 << 20


def stage_orders(size, groups):
    bits = list(range(size.bit_length() - 2, 0, -1))
    low, high = [], []
    for start in range(0, len(bits), 2):
        pair = bits[start : start + 2]
        low += pair if start == 0 else pair[::-1]
        high += pair[::-1] if start == 0 else pair
    half = len(bits) // 2
    other = [[*order[: half - 1], order[half], order[half - 1], *order[half + 1 :]] for order in (low, high)]
    return [other if group % 2 == 1 else [low, high] for group in range(groups)]


def masks_of(order):
    masks = [0]
    for bit in order:
        masks += [mask | (1 << bit) for mask in masks]
    return tuple(masks)


def owner_of(me, masks, block):
    half = len(masks[0])
    core = lax.rem(me, 2)
    if block < half:
        return me ^ jnp.where(core == 0, masks[0][block], masks[1][block])
    block -= half
    return me ^ 1 ^ jnp.where(core == 0, masks[1][block], masks[0][block])


def swap(value, order_pair, stage, size):
    pairs = [(i, i ^ (1 << order_pair[i & 1][stage])) for i in range(size)]
    return lax.ppermute(value, AXIS, pairs)


def swap_core(value, size):
    return lax.ppermute(value, AXIS, [(i, i ^ 1) for i in range(size)])


def stats_kernel(masks, me_ref, teacher_ref, *refs):
    me = me_ref[0]
    groups = teacher_ref.shape[0]
    own_refs, pair_refs, out_ref = refs[:groups], refs[groups : 2 * groups], refs[2 * groups]
    half = len(masks[0][0])
    size = 2 * half
    lane = lax.broadcasted_iota(jnp.int32, (ROW_TILE, groups * size), 1)
    norm_all = jnp.zeros((ROW_TILE, groups * size), jnp.float32)
    mass_all = norm_all
    cross_all = norm_all
    for block in range(size):
        source = own_refs if block < half else pair_refs
        for group in range(groups):
            owner = owner_of(me, masks[group], block)
            start = pl.multiple_of(owner * ROW_TILE, ROW_TILE)
            logits = source[group][pl.ds((block % half) * ROW_TILE, ROW_TILE), :]
            target = teacher_ref[group, pl.ds(start, ROW_TILE), :].astype(jnp.float32)
            peak = jnp.max(logits, axis=1, keepdims=True)
            total = jnp.sum(jnp.exp(logits - peak), axis=1, keepdims=True)
            mass = jnp.sum(target, axis=1, keepdims=True)
            cross = jnp.sum(target * logits, axis=1, keepdims=True)
            here = lane == group * size + owner
            norm_all = jnp.where(here, peak + jnp.log(total), norm_all)
            mass_all = jnp.where(here, mass, mass_all)
            cross_all = jnp.where(here, cross, cross_all)
    out_ref[0] = norm_all
    out_ref[1] = mass_all
    out_ref[2] = cross_all


def grad_kernel(masks, me_ref, stats_ref, teacher_ref, *refs):
    me = me_ref[0]
    groups = teacher_ref.shape[0]
    own_refs, pair_refs = refs[:groups], refs[groups : 2 * groups]
    loss_ref, own_grad_ref, pair_grad_ref = refs[2 * groups :]
    half = len(masks[0][0])
    size = 2 * half
    log_norm, mass, cross = stats_ref[0], stats_ref[1], stats_ref[2]
    loss_ref[...] = mass * log_norm - cross
    lane = lax.broadcasted_iota(jnp.int32, mass.shape, 1)
    for block in range(size):
        source = own_refs if block < half else pair_refs
        result = own_grad_ref if block < half else pair_grad_ref
        for group in range(groups):
            owner = owner_of(me, masks[group], block)
            start = pl.multiple_of(owner * ROW_TILE, ROW_TILE)
            logits = source[group][pl.ds((block % half) * ROW_TILE, ROW_TILE), :]
            here = lane == group * size + owner
            norm_rows = jnp.sum(jnp.where(here, log_norm, 0.0), axis=1, keepdims=True)
            mass_rows = jnp.sum(jnp.where(here, mass, 0.0), axis=1, keepdims=True)
            target = teacher_ref[group, pl.ds(start, ROW_TILE), :].astype(jnp.float32)
            grad = mass_rows * jnp.exp(logits - norm_rows) - target
            result[pl.ds((group * half + block % half) * ROW_TILE, ROW_TILE), :] = grad.astype(jnp.bfloat16)


def own_loss_kernel(me_ref, all_ref, out_ref):
    me = me_ref[0]
    groups = out_ref.shape[0]
    every = all_ref[...]
    size = every.shape[1] // groups
    lane = lax.broadcasted_iota(jnp.int32, every.shape, 1)
    square = (ROW_TILE, ROW_TILE)
    diagonal = lax.broadcasted_iota(jnp.int32, square, 0) == lax.broadcasted_iota(jnp.int32, square, 1)
    for group in range(groups):
        column = jnp.sum(jnp.where(lane == group * size + me, every, 0.0), axis=1, keepdims=True)
        out_ref[pl.ds(group, 1), :] = jnp.sum(jnp.where(diagonal, column, 0.0), axis=0, keepdims=True)


def vmem(count):
    return [pl.BlockSpec(memory_space=pltpu.VMEM)] * count


def call_stats(me, own, pair, teacher, masks):
    groups, size = teacher.shape[0], 2 * len(masks[0][0])
    return pl.pallas_call(
        functools.partial(stats_kernel, masks),
        out_shape=jax.ShapeDtypeStruct((3, ROW_TILE, groups * size), jnp.float32),
        in_specs=[pl.BlockSpec(memory_space=pltpu.SMEM)] + vmem(2 * groups + 1),
        out_specs=vmem(1)[0],
        cost_estimate=pl.CostEstimate(flops=2_000_000, bytes_accessed=2_400_000, transcendentals=400_000),
        compiler_params=pltpu.CompilerParams(vmem_limit_bytes=VMEM_BYTES),
        name="stats",
    )(me, teacher, *own, *pair)


def call_own_loss(me, every, groups):
    return pl.pallas_call(
        own_loss_kernel,
        out_shape=jax.ShapeDtypeStruct((groups, ROW_TILE), jnp.float32),
        in_specs=[pl.BlockSpec(memory_space=pltpu.SMEM)] + vmem(1),
        out_specs=vmem(1)[0],
        cost_estimate=pl.CostEstimate(flops=1000, bytes_accessed=2000, transcendentals=0),
        compiler_params=pltpu.CompilerParams(vmem_limit_bytes=VMEM_BYTES),
        name="own_loss",
    )(me, every)


def call_grad(me, stats, own, pair, teacher, masks):
    groups = len(own)
    grad = jax.ShapeDtypeStruct((groups * own[0].shape[0], own[0].shape[1]), jnp.bfloat16)
    return pl.pallas_call(
        functools.partial(grad_kernel, masks),
        out_shape=[jax.ShapeDtypeStruct(stats.shape[1:], jnp.float32), grad, grad],
        in_specs=[pl.BlockSpec(memory_space=pltpu.SMEM)] + vmem(2 * groups + 2),
        out_specs=vmem(3),
        cost_estimate=pl.CostEstimate(flops=2_000_000, bytes_accessed=3_200_000, transcendentals=400_000),
        compiler_params=pltpu.CompilerParams(vmem_limit_bytes=VMEM_BYTES),
        name="grad",
    )(me, stats, teacher, *own, *pair)


def joined(own, pair, size):
    parts = [jnp.stack(part).reshape(len(part), size // 2, -1, part[0].shape[-1]) for part in (own, pair)]
    return jnp.concatenate(parts, axis=1)


def taken(values, owners):
    return jnp.stack([jnp.take(value, owner, axis=0) for value, owner in zip(values, owners)])


def plain_stats(owners, own, pair, teacher):
    logits = joined(own, pair, teacher.shape[1])
    target = taken(teacher, owners).astype(jnp.float32)
    peak = jnp.max(logits, axis=-1)
    norm = peak + jnp.log(jnp.sum(jnp.exp(logits - peak[..., None]), axis=-1))
    stats = jnp.stack([norm, jnp.sum(target, axis=-1), jnp.sum(target * logits, axis=-1)])
    back = [jnp.zeros_like(stats[:, 0]).at[:, owner].set(stats[:, group]) for group, owner in enumerate(owners)]
    return jnp.stack(back, axis=1)


def plain_grad(me, owners, stats, own, pair, teacher):
    size, _, width = teacher.shape[1:]
    log_norm, mass, cross = stats
    loss = lax.dynamic_index_in_dim(mass * log_norm - cross, me, axis=1, keepdims=False)
    shifted = joined(own, pair, size) - taken(log_norm, owners)[..., None]
    grad = taken(mass, owners)[..., None] * jnp.exp(shifted) - taken(teacher, owners).astype(jnp.float32)
    grad = grad.astype(jnp.bfloat16)
    own_grad, pair_grad = grad[:, : size // 2], grad[:, size // 2 :]
    return loss, own_grad.reshape(-1, width), pair_grad.reshape(-1, width)


def merge_stats(left, right):
    plane = lax.broadcasted_iota(jnp.int32, left.shape, 0)
    high, low = jnp.maximum(left, right), jnp.minimum(left, right)
    return jnp.where(plane == 0, high + jnp.log1p(jnp.exp(low - high)), left + right)


def exchange_stats(stats, size):
    stats = merge_stats(stats, swap_core(stats, size))
    bits = list(range(1, size.bit_length() - 1))
    while bits:
        step, bits = bits[:STATS_RADIX_BITS], bits[STATS_RADIX_BITS:]
        got = [lax.ppermute(stats, AXIS, [(i, i ^ mask) for i in range(size)]) for mask in masks_of(step)[1:]]
        for value in got:
            stats = merge_stats(stats, value)
    return stats


def matmul(left, right, contract):
    return lax.dot_general(left, right, (contract, ((), ())), preferred_element_type=jnp.float32)


def add_round(left, right):
    return (left.astype(jnp.float32) + right.astype(jnp.float32)).astype(jnp.bfloat16)


def shards(hidden, head_weight, teacher):
    groups, row_count, _ = hidden.shape
    size = lax.axis_size(AXIS)
    me = lax.axis_index(AXIS)
    walks = stage_orders(size, groups)
    masks = [[masks_of(order) for order in walk] for walk in walks]
    stages = len(walks[0][0])
    width = head_weight.shape[1]

    held = [hidden[group] for group in range(groups)]
    for stage in range(stages):
        for group in range(groups):
            rows = lax.optimization_barrier(held[group])
            got = swap(rows, walks[group], stage, size)
            held[group] = jnp.concatenate([rows, got])
    held = [lax.optimization_barrier(rows) for rows in held]
    other, own, pair = [], [], []
    for group in range(groups):
        other.append(swap_core(held[group], size))
        own.append(matmul(held[group], head_weight, ((1,), (0,))))
        pair.append(matmul(other[group], head_weight, ((1,), (0,))))

    if row_count == ROW_TILE:
        stats = exchange_stats(call_stats(me.reshape(1), own, pair, teacher, masks), size)
        loss, own_grad, pair_grad = call_grad(me.reshape(1), stats, own, pair, teacher, masks)
        loss = call_own_loss(me.reshape(1), loss, groups)
    else:
        owners = [jnp.stack([owner_of(me, masks[group], block) for block in range(size)]) for group in range(groups)]
        blocks = teacher.reshape(groups, size, row_count, width)
        stats = exchange_stats(plain_stats(owners, own, pair, blocks), size)
        loss, own_grad, pair_grad = plain_grad(me, owners, stats, own, pair, blocks)

    sent = matmul(pair_grad, head_weight, ((1,), (1,))).astype(jnp.bfloat16)
    sent, mine = lax.optimization_barrier((sent, own_grad))
    kept = matmul(mine, head_weight, ((1,), (1,)))
    half = kept.shape[0] // groups
    kept = lax.optimization_barrier([kept[group * half : (group + 1) * half] for group in range(groups)])
    totals = []
    for group in range(groups):
        rows = slice(group * half, (group + 1) * half)
        got = swap_core(sent[rows], size)
        totals.append(add_round(kept[group], got))

    row_blocks = jnp.concatenate([*held, *other])
    grad_blocks = jnp.concatenate([own_grad, pair_grad])
    weight_grad = matmul(row_blocks, grad_blocks, ((0,), (0,)))

    for stage in reversed(range(stages)):
        rows = totals[0].shape[0] // 2
        for group in range(groups):
            got = swap(totals[group][rows:], walks[group], stage, size)
            totals[group] = add_round(totals[group][:rows], got)
    return (loss, jnp.stack(totals), weight_grad.astype(jnp.bfloat16))


def solution(mesh):
    in_specs = (P(None, AXIS, None), P(None, AXIS), P(None, None, AXIS))
    out_specs = (P(None, AXIS), P(None, AXIS, None), P(None, AXIS))

    return jax.shard_map(shards, mesh=mesh, in_specs=in_specs, out_specs=out_specs, check_vma=False)
```

```python
import functools

import jax
import jax.numpy as jnp
from jax import lax
from jax.experimental import pallas as pl
from jax.experimental.pallas import tpu as pltpu
from jax.sharding import PartitionSpec as P

AXIS = "vocab"
ROW_TILE = 8
STATS_RADIX_BITS = 2
VMEM_BYTES = 12 << 20


def stage_orders(size, groups):
    bits = list(range(size.bit_length() - 2, 0, -1))
    half = len(bits) // 2
    walks = []
    for group in range(groups):
        odd = group % 2
        low, high = [], []
        for start in range(0, len(bits), 2):
            pair = bits[start : start + 2]
            turn = odd and start > 0
            low += pair[::-1] if turn else pair
            high += pair if turn else pair[::-1]
        if odd and half:
            for order in (low, high):
                order[half - 1], order[half] = order[half], order[half - 1]
        walks.append([low, high])
    return walks


def masks_of(order):
    masks = [0]
    for bit in order:
        masks += [mask | (1 << bit) for mask in masks]
    return tuple(masks)


def owner_of(me, masks, block):
    half = len(masks[0])
    core = lax.rem(me, 2)
    if block < half:
        return me ^ jnp.where(core == 0, masks[0][block], masks[1][block])
    block -= half
    return me ^ 1 ^ jnp.where(core == 0, masks[1][block], masks[0][block])


def swap(value, order_pair, stage, size):
    pairs = [(i, i ^ (1 << order_pair[i & 1][stage])) for i in range(size)]
    return lax.ppermute(value, AXIS, pairs)


def swap_core(value, size):
    return lax.ppermute(value, AXIS, [(i, i ^ 1) for i in range(size)])


def stats_kernel(masks, me_ref, teacher_ref, *refs):
    me = me_ref[0]
    groups = teacher_ref.shape[0]
    own_refs, pair_refs, out_ref = refs[:groups], refs[groups : 2 * groups], refs[2 * groups]
    half = len(masks[0][0])
    size = 2 * half
    lane = lax.broadcasted_iota(jnp.int32, (ROW_TILE, groups * size), 1)
    norm_all = jnp.zeros((ROW_TILE, groups * size), jnp.float32)
    mass_all = norm_all
    cross_all = norm_all
    for block in range(size):
        source = own_refs if block < half else pair_refs
        for group in range(groups):
            owner = owner_of(me, masks[group], block)
            start = pl.multiple_of(owner * ROW_TILE, ROW_TILE)
            logits = source[group][pl.ds((block % half) * ROW_TILE, ROW_TILE), :]
            target = teacher_ref[group, pl.ds(start, ROW_TILE), :].astype(jnp.float32)
            peak = jnp.max(logits, axis=1, keepdims=True)
            total = jnp.sum(jnp.exp(logits - peak), axis=1, keepdims=True)
            mass = jnp.sum(target, axis=1, keepdims=True)
            cross = jnp.sum(target * logits, axis=1, keepdims=True)
            here = lane == group * size + owner
            norm_all = jnp.where(here, peak + jnp.log(total), norm_all)
            mass_all = jnp.where(here, mass, mass_all)
            cross_all = jnp.where(here, cross, cross_all)
    out_ref[0] = norm_all
    out_ref[1] = mass_all
    out_ref[2] = cross_all


def grad_kernel(masks, me_ref, stats_ref, teacher_ref, *refs):
    me = me_ref[0]
    groups = teacher_ref.shape[0]
    own_refs, pair_refs = refs[:groups], refs[groups : 2 * groups]
    loss_ref, own_grad_ref, pair_grad_ref = refs[2 * groups :]
    half = len(masks[0][0])
    size = 2 * half
    log_norm, mass, cross = stats_ref[0], stats_ref[1], stats_ref[2]
    loss_ref[...] = mass * log_norm - cross
    lane = lax.broadcasted_iota(jnp.int32, mass.shape, 1)
    for block in range(size):
        source = own_refs if block < half else pair_refs
        result = own_grad_ref if block < half else pair_grad_ref
        for group in range(groups):
            owner = owner_of(me, masks[group], block)
            start = pl.multiple_of(owner * ROW_TILE, ROW_TILE)
            logits = source[group][pl.ds((block % half) * ROW_TILE, ROW_TILE), :]
            here = lane == group * size + owner
            norm_rows = jnp.sum(jnp.where(here, log_norm, 0.0), axis=1, keepdims=True)
            mass_rows = jnp.sum(jnp.where(here, mass, 0.0), axis=1, keepdims=True)
            target = teacher_ref[group, pl.ds(start, ROW_TILE), :].astype(jnp.float32)
            grad = mass_rows * jnp.exp(logits - norm_rows) - target
            result[pl.ds((group * half + block % half) * ROW_TILE, ROW_TILE), :] = grad.astype(jnp.bfloat16)


def own_loss_kernel(me_ref, all_ref, out_ref):
    me = me_ref[0]
    groups = out_ref.shape[0]
    every = all_ref[...]
    size = every.shape[1] // groups
    lane = lax.broadcasted_iota(jnp.int32, every.shape, 1)
    square = (ROW_TILE, ROW_TILE)
    diagonal = lax.broadcasted_iota(jnp.int32, square, 0) == lax.broadcasted_iota(jnp.int32, square, 1)
    for group in range(groups):
        column = jnp.sum(jnp.where(lane == group * size + me, every, 0.0), axis=1, keepdims=True)
        out_ref[pl.ds(group, 1), :] = jnp.sum(jnp.where(diagonal, column, 0.0), axis=0, keepdims=True)


def vmem(count):
    return [pl.BlockSpec(memory_space=pltpu.VMEM)] * count


def call_stats(me, own, pair, teacher, masks):
    groups, size = teacher.shape[0], 2 * len(masks[0][0])
    return pl.pallas_call(
        functools.partial(stats_kernel, masks),
        out_shape=jax.ShapeDtypeStruct((3, ROW_TILE, groups * size), jnp.float32),
        in_specs=[pl.BlockSpec(memory_space=pltpu.SMEM)] + vmem(2 * groups + 1),
        out_specs=vmem(1)[0],
        cost_estimate=pl.CostEstimate(flops=2_000_000, bytes_accessed=2_400_000, transcendentals=400_000),
        compiler_params=pltpu.CompilerParams(vmem_limit_bytes=VMEM_BYTES),
        name="stats",
    )(me, teacher, *own, *pair)


def call_own_loss(me, every, groups):
    return pl.pallas_call(
        own_loss_kernel,
        out_shape=jax.ShapeDtypeStruct((groups, ROW_TILE), jnp.float32),
        in_specs=[pl.BlockSpec(memory_space=pltpu.SMEM)] + vmem(1),
        out_specs=vmem(1)[0],
        cost_estimate=pl.CostEstimate(flops=1000, bytes_accessed=2000, transcendentals=0),
        compiler_params=pltpu.CompilerParams(vmem_limit_bytes=VMEM_BYTES),
        name="own_loss",
    )(me, every)


def call_grad(me, stats, own, pair, teacher, masks):
    groups = len(own)
    grad = jax.ShapeDtypeStruct((groups * own[0].shape[0], own[0].shape[1]), jnp.bfloat16)
    return pl.pallas_call(
        functools.partial(grad_kernel, masks),
        out_shape=[jax.ShapeDtypeStruct(stats.shape[1:], jnp.float32), grad, grad],
        in_specs=[pl.BlockSpec(memory_space=pltpu.SMEM)] + vmem(2 * groups + 2),
        out_specs=vmem(3),
        cost_estimate=pl.CostEstimate(flops=2_000_000, bytes_accessed=3_200_000, transcendentals=400_000),
        compiler_params=pltpu.CompilerParams(vmem_limit_bytes=VMEM_BYTES),
        name="grad",
    )(me, stats, teacher, *own, *pair)


def joined(own, pair, size):
    parts = [jnp.stack(part).reshape(len(part), size // 2, -1, part[0].shape[-1]) for part in (own, pair)]
    return jnp.concatenate(parts, axis=1)


def taken(values, owners):
    return jnp.stack([jnp.take(value, owner, axis=0) for value, owner in zip(values, owners)])


def plain_stats(owners, own, pair, teacher):
    logits = joined(own, pair, teacher.shape[1])
    target = taken(teacher, owners).astype(jnp.float32)
    peak = jnp.max(logits, axis=-1)
    norm = peak + jnp.log(jnp.sum(jnp.exp(logits - peak[..., None]), axis=-1))
    stats = jnp.stack([norm, jnp.sum(target, axis=-1), jnp.sum(target * logits, axis=-1)])
    back = [jnp.zeros_like(stats[:, 0]).at[:, owner].set(stats[:, group]) for group, owner in enumerate(owners)]
    return jnp.stack(back, axis=1)


def plain_grad(me, owners, stats, own, pair, teacher):
    size, _, width = teacher.shape[1:]
    log_norm, mass, cross = stats
    loss = lax.dynamic_index_in_dim(mass * log_norm - cross, me, axis=1, keepdims=False)
    shifted = joined(own, pair, size) - taken(log_norm, owners)[..., None]
    grad = taken(mass, owners)[..., None] * jnp.exp(shifted) - taken(teacher, owners).astype(jnp.float32)
    grad = grad.astype(jnp.bfloat16)
    own_grad, pair_grad = grad[:, : size // 2], grad[:, size // 2 :]
    return loss, own_grad.reshape(-1, width), pair_grad.reshape(-1, width)


def merge_stats(left, right):
    plane = lax.broadcasted_iota(jnp.int32, left.shape, 0)
    high, low = jnp.maximum(left, right), jnp.minimum(left, right)
    return jnp.where(plane == 0, high + jnp.log1p(jnp.exp(low - high)), left + right)


def exchange_stats(stats, size):
    stats = merge_stats(stats, swap_core(stats, size))
    bits = list(range(1, size.bit_length() - 1))
    while bits:
        step, bits = bits[:STATS_RADIX_BITS], bits[STATS_RADIX_BITS:]
        got = [lax.ppermute(stats, AXIS, [(i, i ^ mask) for i in range(size)]) for mask in masks_of(step)[1:]]
        for value in got:
            stats = merge_stats(stats, value)
    return stats


def matmul(left, right, contract):
    return lax.dot_general(left, right, (contract, ((), ())), preferred_element_type=jnp.float32)


def add_round(left, right):
    return (left.astype(jnp.float32) + right.astype(jnp.float32)).astype(jnp.bfloat16)


def shards(hidden, head_weight, teacher):
    groups, row_count, _ = hidden.shape
    size = lax.axis_size(AXIS)
    me = lax.axis_index(AXIS)
    walks = stage_orders(size, groups)
    masks = [[masks_of(order) for order in walk] for walk in walks]
    stages = len(walks[0][0])
    width = head_weight.shape[1]

    held = [hidden[group] for group in range(groups)]
    for stage in range(stages):
        for group in range(groups):
            rows = lax.optimization_barrier(held[group])
            got = swap(rows, walks[group], stage, size)
            held[group] = jnp.concatenate([rows, got])
    held = [lax.optimization_barrier(rows) for rows in held]
    other, own, pair = [], [], []
    for group in range(groups):
        other.append(swap_core(held[group], size))
        own.append(matmul(held[group], head_weight, ((1,), (0,))))
        pair.append(matmul(other[group], head_weight, ((1,), (0,))))

    if row_count == ROW_TILE:
        stats = exchange_stats(call_stats(me.reshape(1), own, pair, teacher, masks), size)
        loss, own_grad, pair_grad = call_grad(me.reshape(1), stats, own, pair, teacher, masks)
        loss = call_own_loss(me.reshape(1), loss, groups)
    else:
        owners = [jnp.stack([owner_of(me, masks[group], block) for block in range(size)]) for group in range(groups)]
        blocks = teacher.reshape(groups, size, row_count, width)
        stats = exchange_stats(plain_stats(owners, own, pair, blocks), size)
        loss, own_grad, pair_grad = plain_grad(me, owners, stats, own, pair, blocks)

    sent = matmul(pair_grad, head_weight, ((1,), (1,))).astype(jnp.bfloat16)
    sent, mine = lax.optimization_barrier((sent, own_grad))
    kept = matmul(mine, head_weight, ((1,), (1,)))
    half = kept.shape[0] // groups
    kept = lax.optimization_barrier([kept[group * half : (group + 1) * half] for group in range(groups)])
    totals = []
    for group in range(groups):
        rows = slice(group * half, (group + 1) * half)
        got = swap_core(sent[rows], size)
        totals.append(add_round(kept[group], got))

    row_blocks = jnp.concatenate([*held, *other])
    grad_blocks = jnp.concatenate([own_grad, pair_grad])
    weight_grad = matmul(row_blocks, grad_blocks, ((0,), (0,)))

    for stage in reversed(range(stages)):
        rows = totals[0].shape[0] // 2
        for group in range(groups):
            got = swap(totals[group][rows:], walks[group], stage, size)
            totals[group] = add_round(totals[group][:rows], got)
    return (loss, jnp.stack(totals), weight_grad.astype(jnp.bfloat16))


def solution(mesh):
    in_specs = (P(None, AXIS, None), P(None, AXIS), P(None, None, AXIS))
    out_specs = (P(None, AXIS), P(None, AXIS, None), P(None, AXIS))

    return jax.shard_map(shards, mesh=mesh, in_specs=in_specs, out_specs=out_specs, check_vma=False)
```

```python
import functools

import jax
import jax.numpy as jnp
from jax import lax
from jax.experimental import pallas as pl
from jax.experimental.pallas import tpu as pltpu
from jax.sharding import PartitionSpec as P

AXIS = "vocab"
ROW_TILE = 8
STATS_RADIX_BITS = 2
VMEM_BYTES = 2 << 20


def stage_orders(size, groups):
    bits = list(range(size.bit_length() - 2, 0, -1))
    half = len(bits) // 2
    walks = []
    for group in range(groups):
        odd = group % 2
        low, high = [], []
        for start in range(0, len(bits), 2):
            pair = bits[start : start + 2]
            turn = odd and start > 0
            low += pair if turn else pair[::-1]
            high += pair[::-1] if turn else pair
        if odd and half:
            for order in (low, high):
                order[half - 1], order[half] = order[half], order[half - 1]
        walks.append([low, high])
    return walks


def masks_of(order):
    masks = [0]
    for bit in order:
        masks += [mask | (1 << bit) for mask in masks]
    return tuple(masks)


def owner_of(me, masks, block):
    half = len(masks[0])
    core = lax.rem(me, 2)
    if block < half:
        return me ^ jnp.where(core == 0, masks[0][block], masks[1][block])
    block -= half
    return me ^ 1 ^ jnp.where(core == 0, masks[1][block], masks[0][block])


def swap(value, order_pair, stage, size):
    pairs = [(i, i ^ (1 << order_pair[i & 1][stage])) for i in range(size)]
    return lax.ppermute(value, AXIS, pairs)


def swap_core(value, size):
    return lax.ppermute(value, AXIS, [(i, i ^ 1) for i in range(size)])


def stats_kernel(masks, me_ref, teacher_ref, *refs):
    me = me_ref[0]
    groups = teacher_ref.shape[0]
    own_refs, pair_refs, out_ref = refs[:groups], refs[groups : 2 * groups], refs[2 * groups]
    half = len(masks[0][0])
    size = 2 * half
    lane = lax.broadcasted_iota(jnp.int32, (ROW_TILE, groups * size), 1)
    norm_all = jnp.zeros((ROW_TILE, groups * size), jnp.float32)
    mass_all = norm_all
    cross_all = norm_all
    for block in range(size):
        source = own_refs if block < half else pair_refs
        for group in range(groups):
            owner = owner_of(me, masks[group], block)
            start = pl.multiple_of(owner * ROW_TILE, ROW_TILE)
            logits = source[group][pl.ds((block % half) * ROW_TILE, ROW_TILE), :]
            target = teacher_ref[group, pl.ds(start, ROW_TILE), :].astype(jnp.float32)
            peak = jnp.max(logits, axis=1, keepdims=True)
            total = jnp.sum(jnp.exp(logits - peak), axis=1, keepdims=True)
            mass = jnp.sum(target, axis=1, keepdims=True)
            cross = jnp.sum(target * logits, axis=1, keepdims=True)
            here = lane == group * size + owner
            norm_all = jnp.where(here, peak + jnp.log(total), norm_all)
            mass_all = jnp.where(here, mass, mass_all)
            cross_all = jnp.where(here, cross, cross_all)
    out_ref[0] = norm_all
    out_ref[1] = mass_all
    out_ref[2] = cross_all


def grad_kernel(masks, me_ref, stats_ref, teacher_ref, *refs):
    me = me_ref[0]
    groups = teacher_ref.shape[0]
    own_refs, pair_refs = refs[:groups], refs[groups : 2 * groups]
    loss_ref, own_grad_ref, pair_grad_ref = refs[2 * groups :]
    half = len(masks[0][0])
    size = 2 * half
    log_norm, mass, cross = stats_ref[0], stats_ref[1], stats_ref[2]
    loss_ref[...] = mass * log_norm - cross
    lane = lax.broadcasted_iota(jnp.int32, mass.shape, 1)
    for block in range(size):
        source = own_refs if block < half else pair_refs
        result = own_grad_ref if block < half else pair_grad_ref
        for group in range(groups):
            owner = owner_of(me, masks[group], block)
            start = pl.multiple_of(owner * ROW_TILE, ROW_TILE)
            logits = source[group][pl.ds((block % half) * ROW_TILE, ROW_TILE), :]
            here = lane == group * size + owner
            norm_rows = jnp.sum(jnp.where(here, log_norm, 0.0), axis=1, keepdims=True)
            mass_rows = jnp.sum(jnp.where(here, mass, 0.0), axis=1, keepdims=True)
            target = teacher_ref[group, pl.ds(start, ROW_TILE), :].astype(jnp.float32)
            grad = mass_rows * jnp.exp(logits - norm_rows) - target
            result[pl.ds((group * half + block % half) * ROW_TILE, ROW_TILE), :] = grad.astype(jnp.bfloat16)


def own_loss_kernel(me_ref, all_ref, out_ref):
    me = me_ref[0]
    groups = out_ref.shape[0]
    every = all_ref[...]
    size = every.shape[1] // groups
    lane = lax.broadcasted_iota(jnp.int32, every.shape, 1)
    square = (ROW_TILE, ROW_TILE)
    diagonal = lax.broadcasted_iota(jnp.int32, square, 0) == lax.broadcasted_iota(jnp.int32, square, 1)
    for group in range(groups):
        column = jnp.sum(jnp.where(lane == group * size + me, every, 0.0), axis=1, keepdims=True)
        out_ref[pl.ds(group, 1), :] = jnp.sum(jnp.where(diagonal, column, 0.0), axis=0, keepdims=True)


def vmem(count):
    return [pl.BlockSpec(memory_space=pltpu.VMEM)] * count


def call_stats(me, own, pair, teacher, masks):
    groups, size = teacher.shape[0], 2 * len(masks[0][0])
    return pl.pallas_call(
        functools.partial(stats_kernel, masks),
        out_shape=jax.ShapeDtypeStruct((3, ROW_TILE, groups * size), jnp.float32),
        in_specs=[pl.BlockSpec(memory_space=pltpu.SMEM)] + vmem(2 * groups + 1),
        out_specs=vmem(1)[0],
        cost_estimate=pl.CostEstimate(flops=2_000_000, bytes_accessed=2_400_000, transcendentals=400_000),
        compiler_params=pltpu.CompilerParams(vmem_limit_bytes=VMEM_BYTES),
        name="stats",
    )(me, teacher, *own, *pair)


def call_own_loss(me, every, groups):
    return pl.pallas_call(
        own_loss_kernel,
        out_shape=jax.ShapeDtypeStruct((groups, ROW_TILE), jnp.float32),
        in_specs=[pl.BlockSpec(memory_space=pltpu.SMEM)] + vmem(1),
        out_specs=vmem(1)[0],
        cost_estimate=pl.CostEstimate(flops=1000, bytes_accessed=2000, transcendentals=0),
        compiler_params=pltpu.CompilerParams(vmem_limit_bytes=VMEM_BYTES),
        name="own_loss",
    )(me, every)


def call_grad(me, stats, own, pair, teacher, masks):
    groups = len(own)
    grad = jax.ShapeDtypeStruct((groups * own[0].shape[0], own[0].shape[1]), jnp.bfloat16)
    return pl.pallas_call(
        functools.partial(grad_kernel, masks),
        out_shape=[jax.ShapeDtypeStruct(stats.shape[1:], jnp.float32), grad, grad],
        in_specs=[pl.BlockSpec(memory_space=pltpu.SMEM)] + vmem(2 * groups + 2),
        out_specs=vmem(3),
        cost_estimate=pl.CostEstimate(flops=2_000_000, bytes_accessed=3_200_000, transcendentals=400_000),
        compiler_params=pltpu.CompilerParams(vmem_limit_bytes=VMEM_BYTES),
        name="grad",
    )(me, stats, teacher, *own, *pair)


def joined(own, pair, size):
    parts = [jnp.stack(part).reshape(len(part), size // 2, -1, part[0].shape[-1]) for part in (own, pair)]
    return jnp.concatenate(parts, axis=1)


def taken(values, owners):
    return jnp.stack([jnp.take(value, owner, axis=0) for value, owner in zip(values, owners)])


def plain_stats(owners, own, pair, teacher):
    logits = joined(own, pair, teacher.shape[1])
    target = taken(teacher, owners).astype(jnp.float32)
    peak = jnp.max(logits, axis=-1)
    norm = peak + jnp.log(jnp.sum(jnp.exp(logits - peak[..., None]), axis=-1))
    stats = jnp.stack([norm, jnp.sum(target, axis=-1), jnp.sum(target * logits, axis=-1)])
    back = [jnp.zeros_like(stats[:, 0]).at[:, owner].set(stats[:, group]) for group, owner in enumerate(owners)]
    return jnp.stack(back, axis=1)


def plain_grad(me, owners, stats, own, pair, teacher):
    size, _, width = teacher.shape[1:]
    log_norm, mass, cross = stats
    loss = lax.dynamic_index_in_dim(mass * log_norm - cross, me, axis=1, keepdims=False)
    shifted = joined(own, pair, size) - taken(log_norm, owners)[..., None]
    grad = taken(mass, owners)[..., None] * jnp.exp(shifted) - taken(teacher, owners).astype(jnp.float32)
    grad = grad.astype(jnp.bfloat16)
    own_grad, pair_grad = grad[:, : size // 2], grad[:, size // 2 :]
    return loss, own_grad.reshape(-1, width), pair_grad.reshape(-1, width)


def merge_stats(left, right):
    plane = lax.broadcasted_iota(jnp.int32, left.shape, 0)
    high, low = jnp.maximum(left, right), jnp.minimum(left, right)
    return jnp.where(plane == 0, high + jnp.log1p(jnp.exp(low - high)), left + right)


def exchange_stats(stats, size):
    stats = merge_stats(stats, swap_core(stats, size))
    bits = list(range(1, size.bit_length() - 1))
    while bits:
        step, bits = bits[:STATS_RADIX_BITS], bits[STATS_RADIX_BITS:]
        got = [lax.ppermute(stats, AXIS, [(i, i ^ mask) for i in range(size)]) for mask in masks_of(step)[1:]]
        for value in got:
            stats = merge_stats(stats, value)
    return stats


def matmul(left, right, contract):
    return lax.dot_general(left, right, (contract, ((), ())), preferred_element_type=jnp.float32)


def add_round(left, right):
    return (left.astype(jnp.float32) + right.astype(jnp.float32)).astype(jnp.bfloat16)


def shards(hidden, head_weight, teacher):
    groups, row_count, _ = hidden.shape
    size = lax.axis_size(AXIS)
    me = lax.axis_index(AXIS)
    walks = stage_orders(size, groups)
    masks = [[masks_of(order) for order in walk] for walk in walks]
    stages = len(walks[0][0])
    width = head_weight.shape[1]

    held = [hidden[group] for group in range(groups)]
    for stage in range(stages):
        for group in range(groups):
            rows = lax.optimization_barrier(held[group])
            got = swap(rows, walks[group], stage, size)
            held[group] = jnp.concatenate([rows, got])
    held = [lax.optimization_barrier(rows) for rows in held]
    other, own, pair = [], [], []
    for group in range(groups):
        other.append(swap_core(held[group], size))
        own.append(matmul(held[group], head_weight, ((1,), (0,))))
        pair.append(matmul(other[group], head_weight, ((1,), (0,))))

    if row_count == ROW_TILE:
        stats = exchange_stats(call_stats(me.reshape(1), own, pair, teacher, masks), size)
        loss, own_grad, pair_grad = call_grad(me.reshape(1), stats, own, pair, teacher, masks)
        loss = call_own_loss(me.reshape(1), loss, groups)
    else:
        owners = [jnp.stack([owner_of(me, masks[group], block) for block in range(size)]) for group in range(groups)]
        blocks = teacher.reshape(groups, size, row_count, width)
        stats = exchange_stats(plain_stats(owners, own, pair, blocks), size)
        loss, own_grad, pair_grad = plain_grad(me, owners, stats, own, pair, blocks)

    sent = matmul(pair_grad, head_weight, ((1,), (1,))).astype(jnp.bfloat16)
    sent, mine = lax.optimization_barrier((sent, own_grad))
    kept = matmul(mine, head_weight, ((1,), (1,)))
    half = kept.shape[0] // groups
    kept = lax.optimization_barrier([kept[group * half : (group + 1) * half] for group in range(groups)])
    totals = []
    for group in range(groups):
        rows = slice(group * half, (group + 1) * half)
        got = swap_core(sent[rows], size)
        totals.append(add_round(kept[group], got))

    row_blocks = jnp.concatenate([*held, *other])
    grad_blocks = jnp.concatenate([own_grad, pair_grad])
    weight_grad = matmul(row_blocks, grad_blocks, ((0,), (0,)))

    for stage in reversed(range(stages)):
        rows = totals[0].shape[0] // 2
        for group in range(groups):
            got = swap(totals[group][rows:], walks[group], stage, size)
            totals[group] = add_round(totals[group][:rows], got)
    return (loss, jnp.stack(totals), weight_grad.astype(jnp.bfloat16))


def solution(mesh):
    in_specs = (P(None, AXIS, None), P(None, AXIS), P(None, None, AXIS))
    out_specs = (P(None, AXIS), P(None, AXIS, None), P(None, AXIS))

    return jax.shard_map(shards, mesh=mesh, in_specs=in_specs, out_specs=out_specs, check_vma=False)
```
